256 devices in a mesh: dp: 64 (over z, x, core), mp: 4 (over y).
Axes of the slice: x: 4, y: 4, z: 8, core: 2. Of those that a mesh axis runs over, the one named last changes fastest.
Arguments:
- acts: bfloat16 [16384, 14336], P('dp'), may hold values from -6 to 6
- cotangent: bfloat16 [16384, 2048], P('dp', 'mp'), may hold values from -0.046875 to 0.046875
- stats: float32 [4, 64, 2, 512, 512], P('mp', 'dp'), as said below
- owner_slot: int32 [28], replicated, may hold values from 0 to 63, as said below
Outputs:
- update: bfloat16 [28, 512, 2048], P(None, 'dp', 'mp')
- new_stats: float32 [4, 64, 2, 512, 512], P('mp', 'dp')
The draws below stay inside these ranges and needn't reach their ends.
Inputs may be any that keep to these rules, and one draw needn't show every extreme that they name: Distinct slot numbers; row block w is held by device owner_slot[w] // 1 of dp at its position owner_slot[w] % 1; some device holds 1 block. Every stats[j, s, f] is a symmetric positive definite matrix.
All inputs are finite; a program needn't handle non-finite values.
Results may differ from the reference program's by a relative error of at most 0.012.
The reference program's roundings to bfloat16 on the way (of `gradient`) count: a program that leaves them out, or rounds other values in their place, can miss the bound.
Values may be sent and summed in bfloat16 or wider, within the bound.
No kernel may reach another device: no remote copies, remote signals or barrier semaphores. Data moves between devices by JAX's collectives and lax.ppermute only.
A program may use at most 192 MiB of HBM per device.

```python
import jax
import jax.numpy as jnp
from jax import lax

BLK = 512
SLOTS = 1
ITERS = 5
RB = 28
HID = 14336
COLS = 2048
TOKENS = 16384
N_DP = 64
N_MP = 4


def draw_stats(key, part):
    full_shape = (N_MP, N_DP * SLOTS, 2, BLK, BLK)
    key_off, key_diag = jax.random.split(jax.random.fold_in(key, 11), 2)
    off_noise = 0.1 * jax.random.normal(key_off, full_shape, jnp.float32)
    symmetric = 0.5 * (off_noise + jnp.swapaxes(off_noise, -1, -2))
    identity = jnp.eye(BLK, dtype=jnp.float32)
    off_part = symmetric * (1.0 - identity)
    row_weight = jnp.sum(jnp.abs(off_part), axis=-1)
    dominance = jax.random.uniform(key_diag, full_shape[:-1], jnp.float32, 1.05, 2.0)
    matrix = off_part + identity * (row_weight * dominance)[..., None]
    return matrix


def draw_owner_slot(key, part):
    key_devices, key_places, key_order = jax.random.split(jax.random.fold_in(key, 23), 3)
    holders = RB - SLOTS + 1
    devices = jax.random.permutation(key_devices, N_DP)[:holders].astype(jnp.int32)
    places = jax.random.randint(key_places, (holders,), 0, SLOTS).astype(jnp.int32)
    first_owner = devices[0] * SLOTS + jnp.arange(SLOTS, dtype=jnp.int32)
    other_owners = devices[1:] * SLOTS + places[1:]
    slot_list = jnp.concatenate([first_owner, other_owners])
    shuffle = jax.random.permutation(key_order, RB)
    return slot_list[shuffle].astype(jnp.int32)


def block_scale(rng, shape, shards, smallest, largest):
    loudness = 1.0
    for dim, parts in shards:
        draws = jax.random.uniform(jax.random.fold_in(jax.random.fold_in(rng, 6), dim), (parts,), jnp.float32, smallest / len(shards), largest / len(shards))
        loudness = loudness * jnp.repeat(jnp.exp(draws), shape[dim] // parts).reshape((-1,) + (1,) * (len(shape) - 1 - dim))
    return loudness


def centred(own_key, extent, width, bound, cuts=(), kind=jnp.bfloat16):
    level = block_scale(own_key, extent, cuts, -0.22, 0.18) if cuts else 1.0
    values = jax.random.normal(own_key, extent, jnp.float32) * width * level
    return jnp.minimum(jnp.maximum(values, -bound), bound).astype(kind)


def setup_inputs(seed: int = 0) -> dict:
    streams_of = jax.random.split(jax.random.key(seed), 5)
    return {
        "acts": centred(streams_of[0], (TOKENS, HID), 1.0, 6.0, ((0, 64),)),
        "cotangent": centred(streams_of[1], (TOKENS, COLS), (1.0 / TOKENS ** 0.5), 0.046875, ((0, 64), (1, 4))),
        "stats": draw_stats(jax.random.fold_in(streams_of[4], 71), 0),
        "owner_slot": draw_owner_slot(jax.random.fold_in(streams_of[4], 71), 0),
    }


BETA = 0.9
DAMPING = 0.001
EPSILON = 1e-06

def matmul(former, latter):
    return jnp.dot(former.astype(jnp.bfloat16), latter.astype(jnp.bfloat16), preferred_element_type=jnp.float32)

def inverse_root(statistic):
    identity = jnp.eye(statistic.shape[0], dtype=jnp.float32)
    damped = statistic + DAMPING * identity
    frob_norm = jnp.sqrt(jnp.sum(damped * damped) + EPSILON)
    moment = damped / frob_norm
    result = identity
    for iteration in range(ITERS):
        factor = (5.0 * identity - moment) * 0.25
        if iteration == 0:
            result = factor
        else:
            result = matmul(result, factor)
        if iteration + 1 < ITERS:
            square = matmul(factor, factor)
            moment = matmul(square, matmul(square, moment))
    return result * frob_norm ** (-0.25)

def precondition(grad_block, stat_pair):
    gram_left = jnp.dot(grad_block, grad_block.T, preferred_element_type=jnp.float32)
    gram_right = jnp.dot(grad_block.T, grad_block, preferred_element_type=jnp.float32)
    fresh_left = BETA * stat_pair[0] + (1.0 - BETA) * gram_left
    fresh_right = BETA * stat_pair[1] + (1.0 - BETA) * gram_right
    root_left = inverse_root(fresh_left)
    root_right = inverse_root(fresh_right)
    direction = matmul(matmul(root_left, grad_block), root_right)
    grad_wide = grad_block.astype(jnp.float32)
    graft_ratio = jnp.sqrt((jnp.mean(grad_wide * grad_wide) + EPSILON) / (jnp.mean(direction * direction) + EPSILON))
    return ((direction * graft_ratio).astype(jnp.bfloat16), jnp.stack([fresh_left, fresh_right]))

def reference(acts, cotangent, stats, owner_slot):
    gradient = jnp.dot(acts.T, cotangent, preferred_element_type=jnp.float32).astype(jnp.bfloat16)
    update = jnp.zeros((HID, COLS), jnp.bfloat16)
    zero_index = jnp.zeros((), jnp.int32)

    def one_block(counter, carry):
        stat_store, update_store = carry
        shard = (counter // RB).astype(jnp.int32)
        block_id = (counter % RB).astype(jnp.int32)
        row_start = (block_id * BLK).astype(jnp.int32)
        col_start = (shard * BLK).astype(jnp.int32)
        grad_block = lax.dynamic_slice(gradient, (row_start, col_start), (BLK, BLK))
        slot_id = owner_slot[block_id].astype(jnp.int32)
        stat_pair = lax.dynamic_slice(stat_store, (shard, slot_id, zero_index, zero_index, zero_index), (1, 1, 2, BLK, BLK))[0, 0]
        direction, fresh = precondition(grad_block, stat_pair)
        stat_store = lax.dynamic_update_slice(stat_store, fresh[None, None], (shard, slot_id, zero_index, zero_index, zero_index))
        update_store = lax.dynamic_update_slice(update_store, direction, (row_start, col_start))
        return (stat_store, update_store)
    new_stats, update = lax.fori_loop(0, N_MP * RB, one_block, (stats, update))
    return (update.reshape(RB, BLK, COLS), new_stats)
```

```python
import functools

import jax
import jax.numpy as jnp
from jax import lax
from jax.experimental import pallas as pl
from jax.experimental.pallas import tpu as pltpu
from jax.sharding import Mesh
from jax.sharding import PartitionSpec as P

ITERS = 5
Z, X, C = "dp_0", "dp_1", "dp_2"
DP = (Z, X, C)

BETA = 0.9
DAMPING = 0.001
EPSILON = 1e-06

BF16, F32 = jnp.bfloat16, jnp.float32


def partner(value):
    return lax.ppermute(value, C, [(0, 1), (1, 0)])


def hop(value, axis):
    n = lax.axis_size(axis)
    perm = []
    for i in range(n):
        perm.append((2 * i, 2 * ((i + 1) % n)))
        perm.append((2 * i + 1, 2 * ((i - 1) % n) + 1))
    return lax.ppermute(value, (axis, C), perm)


def partial_kernel(core_ref, lhs_ref, own_ref, other_ref, out_ref):
    k = own_ref.shape[0]
    out_ref[...] = jnp.dot(
        lhs_ref[:, :k], own_ref[...], preferred_element_type=F32
    ) + jnp.dot(lhs_ref[:, k:], other_ref[...], preferred_element_type=F32)


def chip_terms(core, lhs, acts, other, first, step=512):
    cols, depth = lhs.shape
    tokens, rows = other.shape
    half = acts.shape[1] // 2 // step
    return pl.pallas_call(
        partial_kernel,
        grid_spec=pltpu.PrefetchScalarGridSpec(
            num_scalar_prefetch=1,
            grid=(rows // step,),
            in_specs=[
                pl.BlockSpec((cols, depth), lambda i, c: (0, 0)),
                pl.BlockSpec((tokens, step), lambda i, c: (0, c[0] * half + first // step + i)),
                pl.BlockSpec((tokens, step), lambda i, c: (0, i)),
            ],
            out_specs=pl.BlockSpec((cols, step), lambda i, c: (0, i)),
        ),
        out_shape=jax.ShapeDtypeStruct((cols, rows), F32),
        cost_estimate=pl.CostEstimate(
            flops=2 * cols * depth * rows,
            bytes_accessed=4 * cols * rows + 4 * tokens * rows,
            transcendentals=0,
        ),
        name="chip_terms",
    )(core, lhs, acts, other)


class Ring:
    def __init__(self, axis, core, pick):
        self.axis, self.pick = axis, pick
        self.n = lax.axis_size(axis)
        self.me = lax.axis_index(axis)
        self.way = 1 - 2 * core
        self.total = None
        self.sent = 0

    def step(self):
        if self.total is None:
            self.total = self.pick((self.me - self.way) % self.n)
        came = hop(self.total.astype(BF16), self.axis)
        self.sent += 1
        chunk = (self.me - self.way * (self.sent + 1)) % self.n
        self.total = came.astype(F32) + self.pick(chunk)
        return self.sent < self.n - 1


def slots_kernel(core_ref, which_ref, own_ref, other_ref, out_ref, all_ref):
    rows, half = own_ref.shape
    core = core_ref[0]
    block = out_ref.shape[2]
    all_ref[:, pl.ds(pl.multiple_of(core * half, 128), half)] = own_ref[...]
    all_ref[:, pl.ds(pl.multiple_of((1 - core) * half, 128), half)] = other_ref[...]
    for s in range(out_ref.shape[0]):
        w = which_ref[s]
        at = pl.multiple_of(jnp.maximum(w, 0) * block, 128)
        value = all_ref[:, pl.ds(at, block)]
        out_ref[s] = jnp.where(w >= 0, value, jnp.zeros_like(value))


def to_slots(core, which, own, other, block):
    slots = which.shape[0]
    rows, half = own.shape
    smem = pl.BlockSpec(memory_space=pltpu.SMEM)
    vmem = pl.BlockSpec(memory_space=pltpu.VMEM)
    return pl.pallas_call(
        slots_kernel,
        in_specs=[smem, smem, vmem, vmem],
        out_specs=vmem,
        out_shape=jax.ShapeDtypeStruct((slots, rows, block), own.dtype),
        scratch_shapes=[pltpu.VMEM((rows, 2 * half), own.dtype)],
        name="to_slots",
    )(core, which, own, other)


def pick_kernel(slot_ref, came_ref, out_ref):
    for w in range(out_ref.shape[0]):
        out_ref[w] = came_ref[slot_ref[w]]


def pick(slot, came):
    return pl.pallas_call(
        pick_kernel,
        in_specs=[
            pl.BlockSpec(memory_space=pltpu.SMEM),
            pl.BlockSpec(memory_space=pltpu.VMEM),
        ],
        out_specs=pl.BlockSpec(memory_space=pltpu.VMEM),
        out_shape=jax.ShapeDtypeStruct((slot.shape[0], *came.shape[1:]), came.dtype),
        name="pick_rows",
    )(slot, came)


def mm(former, latter, dims=((1,), (0,))):
    return lax.dot_general(former, latter, (dims, ((), ())), preferred_element_type=F32)


def shampoo_kernel(filled_ref, gt_ref, stat_ref, update_ref, new_ref):
    @pl.when(filled_ref[0] == 0)
    def _():
        update_ref[...] = jnp.zeros_like(update_ref)
        new_ref[...] = stat_ref[...]

    @pl.when(filled_ref[0] != 0)
    def _():
        n = gt_ref.shape[0]
        gt = gt_ref[...]
        g = gt.T
        diag = lax.broadcasted_iota(jnp.int32, (n, n), 0) == lax.broadcasted_iota(
            jnp.int32, (n, n), 1
        )
        grams = (mm(g, gt), mm(gt, g))
        norms, moments, results = [], [], []
        for side in range(2):
            fresh = BETA * stat_ref[side] + (1.0 - BETA) * grams[side]
            new_ref[side] = fresh
            damped = fresh + jnp.where(diag, DAMPING, 0.0)
            norm = jnp.sqrt(jnp.sum(damped * damped, keepdims=True) + EPSILON)
            norms.append(norm)
            moments.append(damped / norm)
            results.append(None)
        for k in range(ITERS):
            factors = [
                ((jnp.where(diag, 5.0, 0.0) - m) * 0.25).astype(BF16) for m in moments
            ]
            if k + 1 < ITERS:
                squares = [mm(p, p).astype(BF16) for p in factors]
                inner = [mm(q, m.astype(BF16)).astype(BF16) for q, m in zip(squares, moments)]
            if k == 0:
                results = factors
            else:
                results = [mm(y, p) for y, p in zip(results, factors)]
                if k + 1 < ITERS:
                    results = [y.astype(BF16) for y in results]
            if k + 1 < ITERS:
                moments = [mm(q, i) for q, i in zip(squares, inner)]
        roots = [(y * norm ** (-0.25)).astype(BF16) for y, norm in zip(results, norms)]
        applied = mm(roots[0], g).astype(BF16)
        direction = mm(applied, roots[1])
        wide = gt.astype(F32)
        size = float(n * n)
        ratio = jnp.sqrt(
            (jnp.sum(wide * wide, keepdims=True) / size + EPSILON)
            / (jnp.sum(direction * direction, keepdims=True) / size + EPSILON)
        )
        update_ref[...] = (direction * ratio).astype(BF16)


def shampoo(filled, gt, stat_pair):
    n = gt.shape[0]
    vmem = pl.BlockSpec(memory_space=pltpu.VMEM)
    return pl.pallas_call(
        shampoo_kernel,
        in_specs=[pl.BlockSpec(memory_space=pltpu.SMEM), vmem, vmem],
        out_specs=(vmem, vmem),
        out_shape=(
            jax.ShapeDtypeStruct((n, n), BF16),
            jax.ShapeDtypeStruct(stat_pair.shape, F32),
        ),
        cost_estimate=pl.CostEstimate(
            flops=36 * 2 * n**3, bytes_accessed=20 * n * n, transcendentals=0
        ),
        name="shampoo_block",
    )(filled, gt, stat_pair)


def on_device(acts, cotangent, stats, owner_slot):
    core = lax.axis_index(C)
    core_ref = core.astype(jnp.int32).reshape(1)
    zs, xs = lax.axis_size(Z), lax.axis_size(X)
    blk = cotangent.shape[1]
    rows = acts.shape[1]
    half = rows // 2
    sub = half // 2
    piece = blk // (zs * xs)

    lhs_own = cotangent.T
    lhs = jnp.concatenate([lhs_own, partner(lhs_own)], axis=1)
    terms = []
    for part in range(2):
        away = lax.dynamic_slice(
            acts, (0, (1 - core) * half + part * sub), (acts.shape[0], sub)
        )
        other = partner(away)
        flat = chip_terms(core_ref, lhs, acts, other, part * sub)
        terms.append(flat.reshape(zs, xs, piece, sub))

    first = Ring(Z, core, lambda q: lax.dynamic_index_in_dim(terms[0], q, 0, False))
    second = Ring(X, core, lambda q: lax.dynamic_index_in_dim(terms[1], q, 1, False))
    rings = [first, second]
    done = [None, None]
    while None in done:
        for r in range(2):
            if done[r] is not None:
                continue
            ring = rings[r]
            if not ring.step():
                if (ring.axis == Z) == (r == 0):
                    axis = X if r == 0 else Z
                    rings[r] = Ring(
                        axis,
                        core,
                        functools.partial(
                            lambda whole, q: lax.dynamic_index_in_dim(whole, q, 0, False),
                            ring.total,
                        ),
                    )
                else:
                    done[r] = ring.total.astype(BF16)

    own = jnp.concatenate(done, axis=1)
    other = partner(own)

    chips = jnp.arange(zs * xs, dtype=jnp.int32)
    slots = 2 * chips + core
    held = owner_slot[None, :] == slots[:, None]
    blocks = jnp.arange(owner_slot.shape[0], dtype=jnp.int32)
    which = jnp.sum(jnp.where(held, blocks[None, :] + 1, 0), axis=1) - 1
    outgoing = to_slots(core_ref, which, own, other, blk)
    arrived = lax.all_to_all(outgoing, (Z, X), 0, 0, tiled=True)
    filled = jnp.any(owner_slot == lax.axis_index(DP)).astype(jnp.int32).reshape(1)
    update, new_pair = shampoo(filled, arrived.reshape(blk, blk), stats[0, 0])

    returned = lax.all_to_all(
        update.reshape(2 * zs * xs, piece // 2, blk), DP, 0, 0, tiled=True
    )
    return pick(owner_slot, returned), new_pair[None, None]


def solution(mesh):
    finer = Mesh(mesh.devices.reshape(8, 4, 2, mesh.shape["mp"]), (Z, X, C, "mp"))
    placed = (P(DP, None), P(DP, "mp"), P("mp", DP, None, None, None), P())
    return jax.shard_map(
        on_device,
        mesh=finer,
        in_specs=placed,
        out_specs=(P(None, DP, "mp"), P("mp", DP, None, None, None)),
        check_vma=False,
    )
```
